32 devices in a mesh: row: 4 (over z), col: 8 (over y, x, core).
Axes of the slice: x: 2, y: 2, z: 4, core: 2. Of those that a mesh axis runs over, the one named last changes fastest.
Arguments:
- fine_residual: bfloat16 [16, 524288], P(None, ('row', 'col')), may hold values from -6 to 6
- tiles_one: bfloat16 [8192, 128, 128], P(('row', 'col')), may hold values from -0.1875 to 0.1875
- pointers_one: int32 [4128], P(('row', 'col')), may hold values from 0 to 256, as said below
- columns_one: int32 [8192], P(('row', 'col')), may hold values from 0 to 1023, as said below
- points_one: int32 [131072], P(('col', 'row')), may hold values from 0 to 16383, as said below
- tiles_two: bfloat16 [4096, 128, 128], P(('row', 'col')), may hold values from -0.125 to 0.125
- pointers_two: int32 [2080], P(('row', 'col')), may hold values from 0 to 128, as said below
- columns_two: int32 [4096], P(('row', 'col')), may hold values from 0 to 127
- points_two: int32 [32768], P(('row', 'col')), may hold values from 0 to 4095, as said below
- tiles_three: bfloat16 [512, 128, 128], P(('row', 'col')), may hold values from -0.1875 to 0.1875
- pointers_three: int32 [288], P(('row', 'col')), may hold values from 0 to 16, as said below
- columns_three: int32 [512], P(('row', 'col')), may hold values from 0 to 63
- points_three: int32 [8192], P(('col', 'row')), may hold values from 0 to 1023, as said below
Outputs:
- coarse_one: bfloat16 [16, 131072], P(None, ('col', 'row'))
- coarse_two: bfloat16 [16, 32768], P(None, ('row', 'col'))
- coarse_three: bfloat16 [16, 8192], P(None, ('col', 'row'))
The draws below stay inside these ranges and needn't reach their ends.
Inputs may be any that keep to these rules, and one draw needn't show every extreme that they name: `pointers_one`: each tile set's 128 + 1 pointers start at 0 and never fall; the last is that set's live slot count, at most 256; some set has 256 live slots. `pointers_two`: each tile set's 64 + 1 pointers start at 0 and never fall; the last is that set's live slot count, at most 128; some set has 128 live slots. `pointers_three`: each tile set's 8 + 1 pointers start at 0 and never fall; the last is that set's live slot count, at most 16; some set has 16 live slots. `columns_one`: among the live slots of one tile set, at most 32 name block columns with the same quotient by 128; some set reaches 32. `points_one`: values are distinct within each aligned run of 4096 entries. `points_two`: values are distinct within each aligned run of 1024 entries. `points_three`: values are distinct within each aligned run of 256 entries.
All inputs are finite; a program needn't handle non-finite values.
Results may differ from the reference program's by a relative error of at most 0.0057.
Values may be sent and summed in bfloat16 or wider, within the bound.
No kernel may reach another device: no remote copies, remote signals or barrier semaphores. Data moves between devices by JAX's collectives and lax.ppermute only.
A program may use at most 128 MiB of HBM per device.

```python
import jax
import jax.numpy as jnp
from jax import lax

TILE_EDGE = 128
VECTORS = 16
PIECE_ROWS = 16384
FINE_ROWS = 524288
COARSE_ONE = 131072
COARSE_TWO = 32768
COARSE_THREE = 8192
BLOCKS_ONE = 128
BLOCKS_TWO = 64
BLOCKS_THREE = 8
SLOTS_ONE = 256
SLOTS_TWO = 128
SLOTS_THREE = 16
FINE_BLOCKS_TWO = 128
FINE_BLOCKS_THREE = 64
PEER_SLOTS = 32
N_ROW = 4
N_COL = 8
DEVICES = 32


def live_counts(level_key, slot_count):
    shifts = jax.random.randint(jax.random.fold_in(level_key, 11), (DEVICES,), 0, 5)
    forced = jax.random.randint(jax.random.fold_in(level_key, 12), (), 0, DEVICES)
    shifts = jnp.where(jnp.arange(DEVICES) == forced, 0, shifts)
    full_slots = jnp.full((DEVICES,), slot_count, jnp.int32)
    return jnp.maximum(jnp.right_shift(full_slots, shifts.astype(jnp.int32)), 1).astype(jnp.int32)


def pointer_table(level_key, slot_count, block_count):
    counts = live_counts(level_key, slot_count)
    block_draw = jax.random.randint(jax.random.fold_in(level_key, 13), (DEVICES, slot_count), 0, block_count)
    positions = jnp.arange(slot_count, dtype=jnp.int32)
    block_draw = jnp.where(positions[None, :] < counts[:, None], block_draw, block_count)
    ordered = jnp.sort(block_draw, axis=1)
    bounds = jnp.arange(block_count + 1, dtype=jnp.int32)
    table = jnp.sum((ordered[:, None, :] < bounds[None, :, None]).astype(jnp.int32), axis=2)
    return table.reshape(-1).astype(jnp.int32)


def point_table(level_key, piece_in, piece_out):
    keys = jax.random.split(level_key, DEVICES)
    chosen = jax.vmap(lambda single: jax.random.permutation(single, piece_in)[:piece_out])(keys)
    return chosen.reshape(-1).astype(jnp.int32)


def draw_pointers_one(key, part):
    return pointer_table(jax.random.fold_in(key, 1), SLOTS_ONE, BLOCKS_ONE)


def draw_pointers_two(key, part):
    return pointer_table(jax.random.fold_in(key, 2), SLOTS_TWO, BLOCKS_TWO)


def draw_pointers_three(key, part):
    return pointer_table(jax.random.fold_in(key, 3), SLOTS_THREE, BLOCKS_THREE)


def draw_columns_one(key, part):
    level_key = jax.random.fold_in(key, 1)
    counts = live_counts(level_key, SLOTS_ONE)
    blocks_peer = PIECE_ROWS // TILE_EDGE
    positions = jnp.arange(SLOTS_ONE, dtype=jnp.int32)
    is_live = positions[None, :] < counts[:, None]
    scores = jax.random.randint(jax.random.fold_in(key, 21), (DEVICES, SLOTS_ONE), 0, 1 << 20) * SLOTS_ONE + positions[None, :]
    scores = jnp.where(is_live, scores, scores + (1 << 30))
    rank_order = jnp.argsort(scores, axis=1)
    hot_rank = jnp.argsort(rank_order, axis=1)
    hot_take = jnp.minimum(counts, PEER_SLOTS)
    is_hot = hot_rank < hot_take[:, None]
    hot_peer = jax.random.randint(jax.random.fold_in(key, 22), (DEVICES,), 0, N_COL)
    base_list = jnp.arange((N_COL - 1) * PEER_SLOTS, dtype=jnp.int32) % (N_COL - 1)
    other_keys = jax.random.split(jax.random.fold_in(key, 23), DEVICES)
    others = jax.vmap(lambda single: jax.random.permutation(single, base_list))(other_keys)
    other_rank = jnp.cumsum(1 - is_hot.astype(jnp.int32), axis=1) - 1
    other_rank = jnp.clip(other_rank, 0, (N_COL - 1) * PEER_SLOTS - 1)
    other_choice = jnp.take_along_axis(others, other_rank, axis=1)
    owner_peer = jnp.where(is_hot, hot_peer[:, None], (hot_peer[:, None] + 1 + other_choice) % N_COL)
    offsets = jax.random.randint(jax.random.fold_in(key, 24), (DEVICES, SLOTS_ONE), 0, blocks_peer)
    return (owner_peer * blocks_peer + offsets).reshape(-1).astype(jnp.int32)


def draw_points_one(key, part):
    return point_table(jax.random.fold_in(key, 31), PIECE_ROWS, PIECE_ROWS // 4)


def draw_points_two(key, part):
    return point_table(jax.random.fold_in(key, 32), PIECE_ROWS // 4, PIECE_ROWS // 16)


def draw_points_three(key, part):
    return point_table(jax.random.fold_in(key, 33), PIECE_ROWS // 16, PIECE_ROWS // 64)


def plant(result, own_key, least, largest):
    dims = result.shape
    spot = [jax.random.randint(jax.random.fold_in(own_key, axis), (), 0, dims[axis]) for axis in range(len(dims))]
    result = result.at[tuple(spot)].set(least)
    longest = dims.index(max(dims))
    spot[longest] = (spot[longest] + 1) % dims[longest]
    return result.at[tuple(spot)].set(largest)


def block_scale(rng, extent, cuts, low, high):
    def one(position, blocks):
        draws = jax.random.uniform(jax.random.fold_in(jax.random.fold_in(rng, 6), position), (blocks,), jnp.float32, low / len(cuts), high / len(cuts))
        return jnp.repeat(jnp.exp(draws), extent[position] // blocks).reshape((-1,) + (1,) * (len(extent) - position - 1))

    level = one(*cuts[0])
    for cut in cuts[1:]:
        level = level * one(*cut)
    return level


def gaussian(rng, shape, deviation, most, pieces=(), kind=jnp.bfloat16):
    array = jax.random.normal(rng, shape, jnp.float32) * deviation
    if len(pieces) > 0:
        array = block_scale(rng, shape, pieces, -0.22, 0.18) * array
    return jnp.clip(array, min=-most, max=most).astype(kind)


def setup_inputs(seed: int = 0) -> dict:
    arg_keys = jax.random.split(jax.random.key(seed), 14)
    return {
        "fine_residual": gaussian(arg_keys[0], (VECTORS, FINE_ROWS), 1.0, 6.0, ((1, 32),)),
        "tiles_one": gaussian(arg_keys[1], (DEVICES * SLOTS_ONE, TILE_EDGE, TILE_EDGE), (2 * TILE_EDGE * N_ROW) ** -0.5, 0.1875, ((0, 32),)),
        "pointers_one": draw_pointers_one(jax.random.fold_in(arg_keys[13], 71), 0),
        "columns_one": draw_columns_one(jax.random.fold_in(arg_keys[13], 71), 0),
        "points_one": draw_points_one(jax.random.fold_in(arg_keys[13], 71), 0),
        "tiles_two": gaussian(arg_keys[5], (DEVICES * SLOTS_TWO, TILE_EDGE, TILE_EDGE), (2 * TILE_EDGE * N_COL) ** -0.5, 0.125, ((0, 32),)),
        "pointers_two": draw_pointers_two(jax.random.fold_in(arg_keys[13], 71), 0),
        "columns_two": plant(jax.random.randint(arg_keys[7], (DEVICES * SLOTS_TWO,), 0, FINE_BLOCKS_TWO), jax.random.fold_in(arg_keys[7], 1), 0, FINE_BLOCKS_TWO - 1).astype(jnp.int32),
        "points_two": draw_points_two(jax.random.fold_in(arg_keys[13], 71), 0),
        "tiles_three": gaussian(arg_keys[9], (DEVICES * SLOTS_THREE, TILE_EDGE, TILE_EDGE), (2 * TILE_EDGE * N_ROW) ** -0.5, 0.1875, ((0, 32),)),
        "pointers_three": draw_pointers_three(jax.random.fold_in(arg_keys[13], 71), 0),
        "columns_three": plant(jax.random.randint(arg_keys[11], (DEVICES * SLOTS_THREE,), 0, FINE_BLOCKS_THREE), jax.random.fold_in(arg_keys[11], 1), 0, FINE_BLOCKS_THREE - 1).astype(jnp.int32),
        "points_three": draw_points_three(jax.random.fold_in(arg_keys[13], 71), 0),
    }


def level_tiles(vector, tiles, columns, pointers, slot_count, block_count, fine_size, coarse_size, coarse_total, even_level):
    tile_edge = tiles.shape[1]
    vector_count = vector.shape[0]
    positions = jnp.arange(slot_count, dtype=jnp.int32)

    def one_device(running, device):
        if even_level:
            fine_index = device // N_COL
            coarse_index = device % N_COL
        else:
            fine_index = device % N_COL
            coarse_index = device // N_COL
        my_tiles = lax.dynamic_slice_in_dim(tiles, (device * slot_count).astype(jnp.int32), slot_count, 0).astype(jnp.float32)
        my_columns = lax.dynamic_slice_in_dim(columns, (device * slot_count).astype(jnp.int32), slot_count, 0)
        my_pointers = lax.dynamic_slice_in_dim(pointers, (device * (block_count + 1)).astype(jnp.int32), block_count + 1, 0)
        is_live = positions < my_pointers[block_count]
        finished = jnp.sum((my_pointers[1:][None, :] <= positions[:, None]).astype(jnp.int32), axis=1)
        segment = jnp.where(is_live, finished, block_count).astype(jnp.int32)
        fine_group = lax.dynamic_slice_in_dim(vector, (fine_index * fine_size).astype(jnp.int32), fine_size, 1).astype(jnp.float32)
        blocks = fine_group.reshape(vector_count, fine_size // tile_edge, tile_edge)
        picked = jnp.take(blocks, my_columns, axis=1)
        products = jnp.einsum("sij,vsj->svi", my_tiles, picked, precision=lax.Precision.HIGHEST)
        summed = jax.ops.segment_sum(products, segment, num_segments=block_count + 1)[:block_count]
        part_sum = jnp.transpose(summed, (1, 0, 2)).reshape(vector_count, coarse_size)
        offset = (coarse_index * coarse_size).astype(jnp.int32)
        current = lax.dynamic_slice_in_dim(running, offset, coarse_size, 1)
        return lax.dynamic_update_slice_in_dim(running, current + part_sum, offset, 1), None

    initial = jnp.zeros((vector_count, coarse_total), jnp.float32)
    running, unused = lax.scan(one_device, initial, jnp.arange(DEVICES, dtype=jnp.int32))
    return running


def point_rows(points, piece_in, piece_out, even_level):
    piece_index = jnp.arange(points.shape[0], dtype=jnp.int32) // piece_out
    if even_level:
        grid_row = piece_index % N_ROW
        grid_col = piece_index // N_ROW
        source = grid_row * N_COL + grid_col
    else:
        grid_row = piece_index // N_COL
        grid_col = piece_index % N_COL
        source = grid_col * N_ROW + grid_row
    return (source * piece_in + points).astype(jnp.int32)


def restrict(vector, tiles, columns, pointers, points, slot_count, block_count, fine_size, coarse_size, coarse_total, piece_in, even_level):
    running = level_tiles(vector, tiles, columns, pointers, slot_count, block_count, fine_size, coarse_size, coarse_total, even_level)
    fine_point = point_rows(points, piece_in, coarse_total // DEVICES, even_level)
    injected = jnp.take(vector, fine_point, axis=1).astype(jnp.float32)
    return (running + injected).astype(jnp.bfloat16)


def reference(fine_residual, tiles_one, pointers_one, columns_one, points_one, tiles_two, pointers_two, columns_two, points_two, tiles_three, pointers_three, columns_three, points_three):
    coarse_one = restrict(fine_residual, tiles_one, columns_one, pointers_one, points_one, SLOTS_ONE, BLOCKS_ONE, FINE_ROWS // N_ROW, COARSE_ONE // N_COL, COARSE_ONE, PIECE_ROWS, True)
    coarse_two = restrict(coarse_one, tiles_two, columns_two, pointers_two, points_two, SLOTS_TWO, BLOCKS_TWO, COARSE_ONE // N_COL, COARSE_TWO // N_ROW, COARSE_TWO, PIECE_ROWS // 4, False)
    coarse_three = restrict(coarse_two, tiles_three, columns_three, pointers_three, points_three, SLOTS_THREE, BLOCKS_THREE, COARSE_TWO // N_ROW, COARSE_THREE // N_COL, COARSE_THREE, PIECE_ROWS // 16, True)
    return (coarse_one, coarse_two, coarse_three)
```

```python
import functools
import math

import jax
import jax.numpy as jnp
from jax import lax
from jax.experimental import pallas as pl
from jax.experimental.pallas import tpu as pltpu
from jax.sharding import PartitionSpec as P

F32 = jnp.float32
BF16 = jnp.bfloat16
I32 = jnp.int32
UNROLL = 32

VMEM = pltpu.VMEM
SMEM = pltpu.SMEM


def specs(*spaces):
    return [pl.BlockSpec(memory_space=space) for space in spaces]


def params(*arrays):
    total = sum(jnp.dtype(one.dtype).itemsize * math.prod(one.shape) for one in arrays)
    return pltpu.CompilerParams(vmem_limit_bytes=total * 5 // 4 + (2 << 20))


def exchange(value, axis, count, bit):
    return lax.ppermute(value, axis, [(j, j ^ bit) for j in range(count)])


def segment_kernel(*refs):
    half = len(refs) // 2
    for pointer_ref, segment_ref in zip(refs[:half], refs[half:]):
        blocks = pointer_ref.shape[1] - 1
        slots = segment_ref.shape[1]
        table = pointer_ref[...].astype(F32)
        row = jnp.broadcast_to(table[:, :blocks], (8, blocks))
        eye = (
            lax.broadcasted_iota(I32, (blocks, blocks), 0)
            == lax.broadcasted_iota(I32, (blocks, blocks), 1)
        ).astype(F32)
        column = lax.dot_general(
            eye, row, (((1,), (1,)), ((), ())),
            precision=lax.Precision.HIGHEST, preferred_element_type=F32,
        )[:, :1]
        slot = lax.broadcasted_iota(I32, (blocks, slots), 1).astype(F32)
        begun = jnp.sum(jnp.where(column <= slot, 1.0, 0.0), axis=0, keepdims=True)
        live = slot[:1] < table[:, blocks:]
        segment_ref[...] = jnp.where(live, begun - 1.0, float(blocks)).astype(I32)


def segments(pointer_slots):
    tables = [pointers.reshape(1, -1) for pointers, _ in pointer_slots]
    found = pl.pallas_call(
        segment_kernel,
        out_shape=[jax.ShapeDtypeStruct((1, slots), I32) for _, slots in pointer_slots],
        in_specs=specs(*[VMEM] * len(tables)),
        out_specs=specs(*[VMEM] * len(tables)),
        compiler_params=params(*tables),
        name="segments",
    )(*tables)
    return [one.reshape(-1) for one in found]


def accumulate(live, column_ref, segment_ref, tiles_ref, source, sums):
    unroll = min(UNROLL, tiles_ref.shape[0])
    sums[...] = jnp.zeros(sums.shape, F32)

    def body(step, carry):
        last, running = carry
        products = []
        for offset in range(unroll):
            slot = step * unroll + offset
            products.append(
                lax.dot_general(
                    source[column_ref[slot]], tiles_ref[slot],
                    (((1,), (1,)), ((), ())), preferred_element_type=F32,
                )
            )
        for offset in range(unroll):
            current = segment_ref[step * unroll + offset]
            running = jnp.where(current == last, running, 0.0) + products[offset]
            sums[current] = running
            last = current
        return last, running

    carry = (jnp.int32(-1), jnp.zeros(sums.shape[1:], F32))
    lax.fori_loop(0, (live + unroll - 1) // unroll, body, carry)


def scatter_parts(sums, piece, position, own_ref, send_refs):
    own_ref[...] = sums[pl.ds(position * piece, piece)]
    for index, send_ref in enumerate(send_refs):
        send_ref[...] = sums[pl.ds((position ^ (index + 1)) * piece, piece)].astype(BF16)


def first_kernel(peers, rows, column_ref, segment_ref, pointer_ref, tiles_ref, *refs):
    halves = (len(refs) - rows - 2) // peers
    own_ref = refs[halves * peers]
    sends = refs[halves * peers + 1 : halves * peers + rows]
    source, sums = refs[-2:]
    blocks, thin = refs[0].shape[:2]
    me = lax.axis_index("col")
    for index in range(peers):
        where = pl.ds((me ^ index) * blocks, blocks)
        for half in range(halves):
            piece = refs[half * peers + index]
            source[where, half * thin : (half + 1) * thin, :] = piece[...]
    live = pointer_ref[pointer_ref.shape[0] - 1]
    accumulate(live, column_ref, segment_ref, tiles_ref, source, sums)
    scatter_parts(sums, own_ref.shape[0], lax.axis_index("row"), own_ref, sends)


def first_products(columns, segment, pointers, tiles, halves, rows):
    peers = len(halves[0])
    edge = tiles.shape[1]
    blocks = halves[0][0].shape[0]
    vectors = sum(half[0].shape[1] for half in halves)
    block_rows = pointers.shape[0] - 1
    piece = block_rows // rows
    pieces = [one for half in halves for one in half]
    return pl.pallas_call(
        functools.partial(first_kernel, peers, rows),
        out_shape=[jax.ShapeDtypeStruct((piece, vectors, edge), F32)]
        + [jax.ShapeDtypeStruct((piece, vectors, edge), BF16)] * (rows - 1),
        in_specs=specs(SMEM, SMEM, SMEM, *[VMEM] * (1 + len(pieces))),
        out_specs=specs(*[VMEM] * rows),
        scratch_shapes=[
            pltpu.VMEM((peers * blocks, vectors, edge), BF16),
            pltpu.VMEM((block_rows + 1, vectors, edge), F32),
        ],
        compiler_params=params(
            tiles, *pieces, *pieces, jax.ShapeDtypeStruct((3 * block_rows, vectors, edge), F32)
        ),
        name="first_products",
    )(columns, segment, pointers, tiles, *pieces)


def second_kernel(rows, spread, column_ref, segment_ref, pointer_ref, wanted_ref, tiles_ref, inject_ref, *refs):
    pieces = refs[:rows]
    send_ref, source, sums = refs[rows:]
    blocks = pieces[0].shape[0]
    me = lax.axis_index("row")
    for index, piece in enumerate(pieces):
        source[pl.ds((me ^ index) * blocks, blocks)] = piece[...]
    live = pointer_ref[pointer_ref.shape[0] - 1]
    accumulate(live, column_ref, segment_ref, tiles_ref, source, sums)
    peers = send_ref.shape[0]
    owned = send_ref.shape[1] - spread
    for peer in range(peers):
        send_ref[peer, pl.ds(0, owned)] = sums[pl.ds(peer * owned, owned)].astype(BF16)
    mine = pl.ds(lax.axis_index("col") * owned, owned)
    sums[mine] = sums[mine] + inject_ref[...].astype(F32)
    for peer in range(peers):
        for slot in range(spread):
            send_ref[peer, owned + slot] = sums[wanted_ref[peer * spread + slot]].astype(BF16)


def second_products(columns, segment, pointers, wanted, tiles, inject, pieces, peers):
    rows = len(pieces)
    slots, edge = tiles.shape[0], tiles.shape[1]
    blocks, vectors = pieces[0].shape[0], pieces[0].shape[1]
    block_rows = pointers.shape[0] - 1
    spread = wanted.shape[0] // peers
    return pl.pallas_call(
        functools.partial(second_kernel, rows, spread),
        out_shape=jax.ShapeDtypeStruct((peers, block_rows // peers + spread, vectors, edge), BF16),
        in_specs=specs(SMEM, SMEM, SMEM, SMEM, VMEM, VMEM, *[VMEM] * rows),
        out_specs=pl.BlockSpec(memory_space=VMEM),
        scratch_shapes=[
            pltpu.VMEM((rows * blocks, vectors, edge), BF16),
            pltpu.VMEM((block_rows + 1, vectors, edge), F32),
        ],
        compiler_params=params(
            tiles, *pieces, *pieces, jax.ShapeDtypeStruct((4 * block_rows, vectors, edge), F32)
        ),
        name="second_products",
    )(columns, segment, pointers, wanted, tiles, inject, *pieces)


def third_kernel(rows, segment_ref, pointer_ref, tiles_ref, got_ref, inject_ref, coarse_ref, own_ref, *refs):
    sends = refs[: rows - 1]
    source, order, sums = refs[rows - 1 :]
    peers = got_ref.shape[0]
    owned = inject_ref.shape[0]
    spread = source.shape[0]
    total = got_ref[0].astype(F32)
    for peer in range(1, peers):
        total = total + got_ref[peer].astype(F32)
    edge = got_ref.shape[3]
    for block in range(owned):
        rounded = (total[block] + inject_ref[block].astype(F32)).astype(BF16)
        coarse_ref[:, block * edge : (block + 1) * edge] = rounded
    source[...] = total[owned:].astype(BF16)
    for slot in range(spread):
        order[slot] = slot
    live = pointer_ref[pointer_ref.shape[0] - 1]
    accumulate(live, order, segment_ref, tiles_ref, source, sums)
    scatter_parts(sums, own_ref.shape[0], lax.axis_index("row"), own_ref, sends)


def third_products(segment, pointers, tiles, got, inject, rows):
    slots, edge = tiles.shape[0], tiles.shape[1]
    vectors = got.shape[2]
    block_rows = pointers.shape[0] - 1
    owned = inject.shape[0]
    piece = block_rows // rows
    return pl.pallas_call(
        functools.partial(third_kernel, rows),
        out_shape=[
            jax.ShapeDtypeStruct((vectors, owned * edge), BF16),
            jax.ShapeDtypeStruct((piece, vectors, edge), F32),
        ]
        + [jax.ShapeDtypeStruct((piece, vectors, edge), BF16)] * (rows - 1),
        in_specs=specs(SMEM, SMEM, VMEM, VMEM, VMEM),
        out_specs=specs(*[VMEM] * (rows + 1)),
        scratch_shapes=[
            pltpu.VMEM((slots, vectors, edge), BF16),
            pltpu.SMEM((slots,), I32),
            pltpu.VMEM((block_rows + 1, vectors, edge), F32),
        ],
        compiler_params=params(tiles, got, got, got),
        name="third_products",
    )(segment, pointers, tiles, got, inject)


def add_kernel(own_ref, inject_ref, *refs):
    blocks_ref, rows_ref = refs[-2:]
    edge = own_ref.shape[2]
    for block in range(own_ref.shape[0]):
        total = own_ref[block] + inject_ref[block].astype(F32)
        for part in refs[:-2]:
            total = total + part[block].astype(F32)
        total = total.astype(BF16)
        blocks_ref[block] = total
        rows_ref[:, block * edge : (block + 1) * edge] = total


def add_parts(own, inject, parts, name):
    count, vectors, edge = own.shape
    return pl.pallas_call(
        add_kernel,
        out_shape=[
            jax.ShapeDtypeStruct(own.shape, BF16),
            jax.ShapeDtypeStruct((vectors, count * edge), BF16),
        ],
        in_specs=specs(*[VMEM] * (2 + len(parts))),
        out_specs=specs(VMEM, VMEM),
        compiler_params=params(own, inject, *parts),
        name=name,
    )(own, inject, *parts)


def pick_kernel(width, tile, point_ref, source_ref, out_ref):
    vectors, length = source_ref.shape
    edge = out_ref.shape[2]
    stack = jnp.concatenate(
        [source_ref[:, at : at + width] for at in range(0, length, width)], axis=0
    )
    inner = lax.broadcasted_iota(I32, (width, tile), 0)

    def body(step, carry):
        points = point_ref[:, pl.ds(pl.multiple_of(step * tile, tile), tile)]
        chosen = jnp.where(inner == points % width, 1.0, 0.0).astype(BF16)
        every = jnp.dot(stack, chosen, preferred_element_type=F32)
        group = jnp.broadcast_to(points // width, (vectors, tile))
        total = jnp.zeros((vectors, tile), F32)
        for index in range(length // width):
            total = jnp.where(group == index, every[index * vectors : (index + 1) * vectors], total)
        for block in range(tile // edge):
            out_ref[step * (tile // edge) + block] = total[
                :, block * edge : (block + 1) * edge
            ].astype(BF16)
        return carry

    lax.fori_loop(0, point_ref.shape[1] // tile, body, 0)


def pick_points(points, source, edge, width, tile, name):
    vectors = source.shape[0]
    count = points.shape[0]
    return pl.pallas_call(
        functools.partial(pick_kernel, width, min(tile, count)),
        out_shape=jax.ShapeDtypeStruct((count // edge, vectors, edge), BF16),
        in_specs=specs(VMEM, VMEM),
        out_specs=pl.BlockSpec(memory_space=VMEM),
        compiler_params=pltpu.CompilerParams(vmem_limit_bytes=16 << 20),
        name=name,
    )(points.reshape(1, -1), source)


def to_blocks(rows, edge):
    vectors, wide = rows.shape
    return jnp.transpose(rows.reshape(vectors, wide // edge, edge), (1, 0, 2))


def gather_pieces(piece, axis, count, reverse):
    bits = []
    bit = count // 2
    while bit > 1:
        bits.append(bit)
        bit //= 2
    if reverse:
        bits = bits[::-1]
    bits.append(1)
    pieces = {0: piece}
    for bit in bits:
        if bit < count:
            for index in list(pieces):
                pieces[index ^ bit] = exchange(pieces[index], axis, count, bit)
    return [pieces[index] for index in range(count)]


def on_device(
    fine_residual,
    tiles_one,
    pointers_one,
    columns_one,
    points_one,
    tiles_two,
    pointers_two,
    columns_two,
    points_two,
    tiles_three,
    pointers_three,
    columns_three,
    points_three,
):
    rows = lax.axis_size("row")
    peers = lax.axis_size("col")
    edge = tiles_one.shape[1]
    thin = fine_residual.shape[0] // 2
    halves = [
        gather_pieces(to_blocks(fine_residual[h * thin : (h + 1) * thin], edge), "col", peers, h == 1)
        for h in range(2)
    ]
    wanted = lax.all_gather(columns_three, "col", axis=0, tiled=True)
    segment_one, segment_two, segment_three = segments(
        [
            (pointers_one, tiles_one.shape[0]),
            (pointers_two, tiles_two.shape[0]),
            (pointers_three, tiles_three.shape[0]),
        ]
    )
    inject = pick_points(points_one, fine_residual, edge, 2 * edge, 4 * edge, "points_one")
    wanted, inject, halves = lax.optimization_barrier((wanted, inject, halves))
    own, *sends = first_products(columns_one, segment_one, pointers_one, tiles_one, halves, rows)
    got = [exchange(send, "row", rows, k + 1) for k, send in enumerate(sends)]
    blocks, coarse_one = add_parts(own, inject, got, "coarse_one")
    spread = [blocks] + [exchange(blocks, "row", rows, k) for k in range(1, rows)]
    inject = pick_points(points_two, coarse_one, edge, 2 * edge, 4 * edge, "points_two")
    send = second_products(
        columns_two, segment_two, pointers_two, wanted, tiles_two, inject, spread, peers
    )
    got = lax.all_to_all(send, "col", split_axis=0, concat_axis=0, tiled=True)
    coarse_two, own, *sends = third_products(
        segment_three, pointers_three, tiles_three, got, inject, rows
    )
    got = [exchange(send, "row", rows, k + 1) for k, send in enumerate(sends)]
    inject = pick_points(points_three, coarse_two, edge, edge, 4 * edge, "points_three")
    coarse_three = add_parts(own, inject, got, "coarse_three")[1]
    return coarse_one, coarse_two, coarse_three


def solution(mesh):
    placed = (
        P(None, ("row", "col")),
        P(("row", "col"), None, None),
        P(("row", "col")),
        P(("row", "col")),
        P(("col", "row")),
        P(("row", "col"), None, None),
        P(("row", "col")),
        P(("row", "col")),
        P(("row", "col")),
        P(("row", "col"), None, None),
        P(("row", "col")),
        P(("row", "col")),
        P(("col", "row")),
    )
    return jax.shard_map(
        on_device,
        mesh=mesh,
        in_specs=placed,
        out_specs=(P(None, ("col", "row")), P(None, ("row", "col")), P(None, ("col", "row"))),
        check_vma=False,
    )
```

```python
import functools
import math

import jax
import jax.numpy as jnp
from jax import lax
from jax.experimental import pallas as pl
from jax.experimental.pallas import tpu as pltpu
from jax.sharding import PartitionSpec as P


F32 = jnp.float32
BF16 = jnp.bfloat16
I32 = jnp.int32
UNROLL = 64
COST = 8 * 10**9


VMEM = pltpu.VMEM
SMEM = pltpu.SMEM


def specs(*spaces):
    return [pl.BlockSpec(memory_space=space) for space in spaces]


def params(*arrays):
    total = sum(jnp.dtype(one.dtype).itemsize * math.prod(one.shape) for one in arrays)
    return pltpu.CompilerParams(vmem_limit_bytes=total * 5 // 4 + (2 << 20))


def exchange(value, axis, count, bit):
    return lax.ppermute(value, axis, [(j, j ^ bit) for j in range(count)])


def section(slots):
    return (slots + 127) // 128 * 128


def table_kernel(levels, *refs):
    count = 2 * levels - 1
    table_refs = refs[count : count + levels]
    fetched = refs[:count]
    for level, table_ref in enumerate(table_refs):
        pointers = fetched[level][...].astype(F32)
        blocks = pointers.shape[1] - 1
        wide = (table_ref.shape[1] - 128) // 2
        slots = fetched[levels + level].shape[1] if level < levels - 1 else wide
        row = jnp.broadcast_to(pointers[:, :blocks], (8, blocks))
        eye = (
            lax.broadcasted_iota(I32, (blocks, blocks), 0)
            == lax.broadcasted_iota(I32, (blocks, blocks), 1)
        ).astype(F32)
        column = lax.dot_general(
            eye, row, (((1,), (1,)), ((), ())),
            precision=lax.Precision.HIGHEST, preferred_element_type=F32,
        )[:, :1]
        slot = lax.broadcasted_iota(I32, (blocks, slots), 1)
        begun = jnp.sum(jnp.where(column <= slot.astype(F32), 1.0, 0.0), axis=0, keepdims=True)
        live = pointers[:, blocks:]
        table_ref[...] = jnp.broadcast_to(live, table_ref.shape).astype(I32)
        table_ref[:, :slots] = fetched[levels + level][...] if level < levels - 1 else slot[:1]
        table_ref[:, wide : wide + slots] = jnp.where(
            slot[:1].astype(F32) < live, begun - 1.0, float(blocks)
        ).astype(I32)


def slot_tables(pointers, columns, slots):
    arrays = [one.reshape(1, -1) for one in (*pointers, *columns)]
    shapes = [jax.ShapeDtypeStruct((1, 2 * section(count) + 128), I32) for count in slots]
    return pl.pallas_call(
        functools.partial(table_kernel, len(slots)),
        out_shape=shapes,
        in_specs=specs(*[VMEM] * len(arrays)),
        out_specs=specs(*[VMEM] * len(slots)),
        compiler_params=params(*shapes),
        cost_estimate=pl.CostEstimate(flops=COST, bytes_accessed=COST // 100, transcendentals=0),
        name="slot_tables",
    )(*arrays)


def pack_kernel(offset, fine_ref, *refs):
    out_ref = refs[-1]
    thin, edge = out_ref.shape[1:]
    blocks = fine_ref.shape[1] // edge
    for block in range(blocks):
        out_ref[block] = fine_ref[offset : offset + thin, block * edge : (block + 1) * edge]
    if len(refs) > 1:
        column_ref = refs[0]
        slots = column_ref.shape[1]
        out_ref[blocks] = jnp.zeros((thin, edge), BF16)
        out_ref[blocks, :, :slots] = jnp.broadcast_to(
            column_ref[...].astype(F32), (thin, slots)
        ).astype(BF16)


def pack_fine(fine, offset, edge, extra):
    thin, blocks = fine.shape[0] // 2, fine.shape[1] // edge
    extra = [one.reshape(1, -1) for one in extra]
    return pl.pallas_call(
        functools.partial(pack_kernel, offset),
        out_shape=jax.ShapeDtypeStruct((blocks + len(extra), thin, edge), BF16),
        in_specs=specs(*[VMEM] * (1 + len(extra))),
        out_specs=pl.BlockSpec(memory_space=VMEM),
        compiler_params=params(fine, fine),
        name="pack_fine",
    )(fine, *extra)


def accumulate(table_ref, tiles_ref, fetch, sums):
    slots = tiles_ref.shape[0]
    unroll = min(UNROLL, slots)
    wide = section(slots)
    sums[...] = jnp.zeros(sums.shape, F32)

    def body(step, carry):
        last, running = carry
        products = []
        for offset in range(unroll):
            slot = step * unroll + offset
            products.append(
                lax.dot_general(
                    fetch(table_ref[0, slot]), tiles_ref[slot],
                    (((1,), (1,)), ((), ())), preferred_element_type=F32,
                )
            )
        for offset in range(unroll):
            current = table_ref[0, wide + step * unroll + offset]
            running = jnp.where(current == last, running, 0.0) + products[offset]
            sums[current] = running
            last = current
        return last, running

    carry = (jnp.int32(-1), jnp.zeros(sums.shape[1:], F32))
    lax.fori_loop(0, (table_ref[0, 2 * wide] + unroll - 1) // unroll, body, carry)


def scatter_parts(sums, piece, position, own_ref, send_refs):
    own_ref[...] = sums[pl.ds(position * piece, piece)]
    for index, send_ref in enumerate(send_refs):
        send_ref[...] = sums[pl.ds((position ^ (index + 1)) * piece, piece)].astype(BF16)


def first_kernel(peers, rows, table_ref, tiles_ref, *refs):
    first, second = refs[:peers], refs[peers : 2 * peers]
    wanted_ref, own_ref = refs[2 * peers : 2 * peers + 2]
    sends = refs[2 * peers + 2 : 2 * peers + 1 + rows]
    low, high, sums = refs[-3:]
    blocks = first[0].shape[0]
    me = lax.axis_index("col")
    for index in range(peers):
        where = pl.ds((me ^ index) * blocks, blocks)
        low[where] = first[index][...]
        high[where] = second[index][pl.ds(0, blocks)]
        wanted_ref[pl.ds(me ^ index, 1), :] = second[index][blocks].astype(F32)[:1].astype(I32)

    def fetch(column):
        return jnp.concatenate([low[column], high[column]], axis=0)

    accumulate(table_ref, tiles_ref, fetch, sums)
    scatter_parts(sums, own_ref.shape[0], lax.axis_index("row"), own_ref, sends)


def first_products(table, tiles, halves, rows, block_rows):
    peers = len(halves[0])
    edge = tiles.shape[1]
    blocks, thin = halves[0][0].shape[:2]
    vectors = 2 * thin
    piece = block_rows // rows
    pieces = [one for half in halves for one in half]
    return pl.pallas_call(
        functools.partial(first_kernel, peers, rows),
        out_shape=[
            jax.ShapeDtypeStruct((peers, edge), I32),
            jax.ShapeDtypeStruct((piece, vectors, edge), F32),
        ]
        + [jax.ShapeDtypeStruct((piece, vectors, edge), BF16)] * (rows - 1),
        in_specs=specs(SMEM, *[VMEM] * (1 + len(pieces))),
        out_specs=specs(*[VMEM] * (rows + 1)),
        scratch_shapes=[
            pltpu.VMEM((peers * blocks, thin, edge), BF16),
            pltpu.VMEM((peers * blocks, thin, edge), BF16),
            pltpu.VMEM((block_rows + 1, vectors, edge), F32),
        ],
        compiler_params=params(
            *pieces, jax.ShapeDtypeStruct((block_rows + 1, vectors, edge), F32)
        ),
        name="first_products",
    )(table, tiles, *pieces)


def second_kernel(rows, spread, table_ref, wanted_ref, tiles_ref, inject_ref, *refs):
    pieces = refs[:rows]
    keep_ref, give_ref, source, sums = refs[rows:]
    blocks = pieces[0].shape[0]
    row = lax.axis_index("row")
    for index, piece in enumerate(pieces):
        source[pl.ds((row ^ index) * blocks, blocks)] = piece[...]
    accumulate(table_ref, tiles_ref, lambda column: source[column], sums)
    me = lax.axis_index("col")
    owned = keep_ref.shape[1] - spread
    pairs = keep_ref.shape[0]
    for pair in range(pairs):
        for other, target in ((0, keep_ref), (1, give_ref)):
            peer = me ^ (2 * pair + other)
            target[pair, pl.ds(0, owned)] = sums[pl.ds(peer * owned, owned)].astype(target.dtype)
    mine = pl.ds(me * owned, owned)
    sums[mine] = sums[mine] + inject_ref[...].astype(F32)
    for pair in range(pairs):
        for other, target in ((0, keep_ref), (1, give_ref)):
            peer = me ^ (2 * pair + other)
            for slot in range(spread):
                target[pair, owned + slot] = sums[wanted_ref[peer, slot]].astype(target.dtype)


def second_products(table, wanted, spread, tiles, inject, pieces, peers, block_rows):
    rows = len(pieces)
    edge = tiles.shape[1]
    blocks, vectors = pieces[0].shape[0], pieces[0].shape[1]
    shape = (peers // 2, block_rows // peers + spread, vectors, edge)
    send = [jax.ShapeDtypeStruct(shape, F32), jax.ShapeDtypeStruct(shape, BF16)]
    return pl.pallas_call(
        functools.partial(second_kernel, rows, spread),
        out_shape=send,
        in_specs=specs(SMEM, SMEM, VMEM, VMEM, *[VMEM] * rows),
        out_specs=specs(VMEM, VMEM),
        scratch_shapes=[
            pltpu.VMEM((rows * blocks, vectors, edge), BF16),
            pltpu.VMEM((block_rows + 1, vectors, edge), F32),
        ],
        compiler_params=params(
            *pieces, *send, jax.ShapeDtypeStruct((block_rows + 1, vectors, edge), F32)
        ),
        name="second_products",
    )(table, wanted, tiles, inject, *pieces)


def pair_kernel(keep_ref, got_ref, own_ref, *send_refs):
    for pair in range(keep_ref.shape[0]):
        total = keep_ref[pair] + got_ref[pair].astype(F32)
        if pair == 0:
            own_ref[...] = total
        else:
            send_refs[pair - 1][...] = total.astype(BF16)


def pair_sums(keep, got):
    shape = keep.shape[1:]
    pairs = keep.shape[0]
    return pl.pallas_call(
        pair_kernel,
        out_shape=[jax.ShapeDtypeStruct(shape, F32)]
        + [jax.ShapeDtypeStruct(shape, BF16)] * (pairs - 1),
        in_specs=specs(VMEM, VMEM),
        out_specs=specs(*[VMEM] * pairs),
        compiler_params=params(keep, got, keep),
        name="pair_sums",
    )(keep, got)


def third_kernel(rows, count, table_ref, tiles_ref, inject_ref, *refs):
    parts = refs[:count]
    coarse_ref, own_ref = refs[count : count + 2]
    sends = refs[count + 2 : count + 1 + rows]
    source, sums = refs[-2:]
    owned = inject_ref.shape[0]
    total = parts[0][...]
    for part in parts[1:]:
        total = total + part[...].astype(F32)
    edge = total.shape[2]
    for block in range(owned):
        rounded = (total[block] + inject_ref[block].astype(F32)).astype(BF16)
        coarse_ref[:, block * edge : (block + 1) * edge] = rounded
    source[...] = total[owned:].astype(BF16)
    accumulate(table_ref, tiles_ref, lambda column: source[column], sums)
    scatter_parts(sums, own_ref.shape[0], lax.axis_index("row"), own_ref, sends)


def third_products(table, tiles, parts, inject, rows, block_rows):
    slots, edge = tiles.shape[0], tiles.shape[1]
    vectors = parts[0].shape[1]
    owned = inject.shape[0]
    piece = block_rows // rows
    return pl.pallas_call(
        functools.partial(third_kernel, rows, len(parts)),
        out_shape=[
            jax.ShapeDtypeStruct((vectors, owned * edge), BF16),
            jax.ShapeDtypeStruct((piece, vectors, edge), F32),
        ]
        + [jax.ShapeDtypeStruct((piece, vectors, edge), BF16)] * (rows - 1),
        in_specs=specs(SMEM, *[VMEM] * (2 + len(parts))),
        out_specs=specs(*[VMEM] * (rows + 1)),
        scratch_shapes=[
            pltpu.VMEM((slots, vectors, edge), BF16),
            pltpu.VMEM((block_rows + 1, vectors, edge), F32),
        ],
        compiler_params=params(*parts, *parts),
        name="third_products",
    )(table, tiles, inject, *parts)


def add_kernel(own_ref, inject_ref, *refs):
    blocks_ref, rows_ref = refs[-2:]
    edge = own_ref.shape[2]
    for block in range(own_ref.shape[0]):
        total = own_ref[block] + inject_ref[block].astype(F32)
        for part in refs[:-2]:
            total = total + part[block].astype(F32)
        total = total.astype(BF16)
        blocks_ref[block] = total
        rows_ref[:, block * edge : (block + 1) * edge] = total


def add_parts(own, inject, parts):
    count, vectors, edge = own.shape
    return pl.pallas_call(
        add_kernel,
        out_shape=[
            jax.ShapeDtypeStruct(own.shape, BF16),
            jax.ShapeDtypeStruct((vectors, count * edge), BF16),
        ],
        in_specs=specs(*[VMEM] * (2 + len(parts))),
        out_specs=specs(VMEM, VMEM),
        compiler_params=params(own, inject, *parts),
    )(own, inject, *parts)


def pick_kernel(width, tile, point_ref, source_ref, out_ref):
    vectors, length = source_ref.shape
    edge = out_ref.shape[2]
    stack = jnp.concatenate(
        [source_ref[:, at : at + width] for at in range(0, length, width)], axis=0
    )
    inner = lax.broadcasted_iota(I32, (width, tile), 0)

    def body(step, carry):
        points = point_ref[:, pl.ds(pl.multiple_of(step * tile, tile), tile)]
        chosen = jnp.where(inner == points % width, 1.0, 0.0).astype(BF16)
        every = jnp.dot(stack, chosen, preferred_element_type=F32)
        group = jnp.broadcast_to(points // width, (vectors, tile))
        total = jnp.zeros((vectors, tile), F32)
        for index in range(length // width):
            total = jnp.where(group == index, every[index * vectors : (index + 1) * vectors], total)
        for block in range(tile // edge):
            out_ref[step * (tile // edge) + block] = total[
                :, block * edge : (block + 1) * edge
            ].astype(BF16)
        return carry

    lax.fori_loop(0, point_ref.shape[1] // tile, body, 0)


def pick_points(points, source, edge, width, tile):
    vectors = source.shape[0]
    count = points.shape[0]
    return pl.pallas_call(
        functools.partial(pick_kernel, width, min(tile, count)),
        out_shape=jax.ShapeDtypeStruct((count // edge, vectors, edge), BF16),
        in_specs=specs(VMEM, VMEM),
        out_specs=pl.BlockSpec(memory_space=VMEM),
        compiler_params=pltpu.CompilerParams(vmem_limit_bytes=16 << 20),
    )(points.reshape(1, -1), source)


def high_bits(count, reverse):
    bits = []
    bit = count // 2
    while bit > 1:
        bits.append(bit)
        bit //= 2
    return bits[::-1] if reverse else bits


def gather_pieces(piece, later, got, axis, count, reverse):
    bits = high_bits(count, reverse)
    pieces = {0: piece, bits[0]: got}
    for bit in bits[1:]:
        for index in list(pieces):
            pieces[index ^ bit] = exchange(pieces[index] if index else later, axis, count, bit)
    for index in list(pieces):
        pieces[index ^ 1] = exchange(pieces[index] if index else later, axis, count, 1)
    return [pieces[index] for index in range(count)]


def on_device(
    fine_residual,
    tiles_one,
    pointers_one,
    columns_one,
    points_one,
    tiles_two,
    pointers_two,
    columns_two,
    points_two,
    tiles_three,
    pointers_three,
    columns_three,
    points_three,
):
    rows = lax.axis_size("row")
    peers = lax.axis_size("col")
    edge = tiles_one.shape[1]
    block_rows = [one.shape[0] - 1 for one in (pointers_one, pointers_two, pointers_three)]
    assert block_rows[1] <= 256
    tables = list(slot_tables(
        (pointers_one, pointers_two, pointers_three),
        (columns_one, columns_two),
        (tiles_one.shape[0], tiles_two.shape[0], tiles_three.shape[0]),
    ))
    first = pack_fine(fine_residual, 0, edge, [])
    second = pack_fine(fine_residual, fine_residual.shape[0] // 2, edge, [columns_three])
    starts = [
        exchange(first, "col", peers, high_bits(peers, False)[0]),
        exchange(second, "col", peers, high_bits(peers, True)[0]),
    ]
    later, tables = lax.optimization_barrier(((first, second), tables))
    halves = [
        gather_pieces(half, held, got, "col", peers, name == "b")
        for half, held, got, name in zip((first, second), later, starts, "ab")
    ]
    table_one, table_two, table_three = tables
    wanted, own, *sends = first_products(table_one, tiles_one, halves, rows, block_rows[0])
    got = [exchange(send, "row", rows, k + 1) for k, send in enumerate(sends)]
    fine, own = lax.optimization_barrier((fine_residual, own))
    inject = pick_points(points_one, fine, edge, 2 * edge, 4 * edge)
    blocks, coarse_one = add_parts(own, inject, got)
    pieces = [blocks] + [exchange(blocks, "row", rows, k) for k in range(1, rows)]
    inject = pick_points(points_two, coarse_one, edge, 2 * edge, 4 * edge)
    keep, give = second_products(
        table_two, wanted, tiles_three.shape[0], tiles_two, inject, pieces, peers, block_rows[1]
    )
    own, *sends = pair_sums(keep, exchange(give, "col", peers, 1))
    got = [own] + [exchange(send, "col", peers, 2 * k + 2) for k, send in enumerate(sends)]
    coarse_two, own, *sends = third_products(
        table_three, tiles_three, got, inject, rows, block_rows[2]
    )
    got = [exchange(send, "row", rows, k + 1) for k, send in enumerate(sends)]
    inject = pick_points(points_three, coarse_two, edge, edge, 4 * edge)
    coarse_three = add_parts(own, inject, got)[1]
    return coarse_one, coarse_two, coarse_three


def solution(mesh):
    placed = (
        P(None, ("row", "col")),
        P(("row", "col"), None, None),
        P(("row", "col")),
        P(("row", "col")),
        P(("col", "row")),
        P(("row", "col"), None, None),
        P(("row", "col")),
        P(("row", "col")),
        P(("row", "col")),
        P(("row", "col"), None, None),
        P(("row", "col")),
        P(("row", "col")),
        P(("col", "row")),
    )

    return jax.shard_map(
        on_device,
        mesh=mesh,
        in_specs=placed,
        out_specs=(P(None, ("col", "row")), P(None, ("row", "col")), P(None, ("col", "row"))),
        check_vma=False,
    )
```
